32 devices in a mesh: section: 4 (over z), batch: 2 (over x), tile: 4 (over y, core).
Axes of the slice: x: 2, y: 2, z: 4, core: 2. Of those that a mesh axis runs over, the one named last changes fastest.
Arguments:
- latents: bfloat16 [8, 4, 32, 1280], P('batch', 'tile'), parts along dimension 0, may hold values from -6 to 6
- prompt_tokens: bfloat16 [8, 77, 2048], P('batch'), parts along dimension 0, may hold values from -6 to 6
- fresh_noise: bfloat16 [1, 8, 4, 32, 1280], P(None, 'batch', 'tile'), parts along dimension 1, may hold values from -6 to 6
- timesteps: int32 [2], replicated, may hold values from 600 to 999
- entry_order: int32 [8], P('batch'), parts along dimension 0, may hold values from 0 to 3, each once
- timestep_weight: bfloat16 [4, 320, 1280], P('section'), may hold values from -0.3125 to 0.3125
- conv_kernel: float32 [4, 9, 1280], P('section'), may hold values from -1 to 1
- norm_gain: float32 [4, 1280], P('section'), may hold values from 0.25 to 1.75
- layer_norm_bias: float32 [4, 1280], P('section'), may hold values from -1.5 to 1.5
- qkv_weight: bfloat16 [4, 1280, 3, 1280], P('section', None, None, 'tile'), may hold values from -0.15625 to 0.15625
- prompt_weight: bfloat16 [4, 2048, 2, 1280], P('section', None, None, 'tile'), may hold values from -0.125 to 0.125
- out_weight: bfloat16 [4, 1280, 1280], P('section', 'tile'), may hold values from -0.15625 to 0.15625
Outputs:
- samples: bfloat16 [8, 4, 32, 1280], P('batch', 'tile', None, 'section'), parts along dimension 0
The draws below stay inside these ranges and needn't reach their ends.
There are 2 independent parts, one for each index of `batch`. The reference program is written for one: setup_inputs(seed, part) draws one part's arguments, and reference() takes and returns one part's arrays. A program takes and returns all parts, laid end to end along the dimension named above; an argument that names none is the same for every part. Nothing has to cross between parts.
All inputs are finite; a program needn't handle non-finite values.
Results may differ from the reference program's by a relative error of at most 0.019.
Values may be sent and summed in bfloat16 or wider, within the bound.
No kernel may reach another device: no remote copies, remote signals or barrier semaphores. Data moves between devices by JAX's collectives and lax.ppermute only.
A program may use at most 64 MiB of HBM per device.

```python
import math
import jax
import jax.numpy as jnp
from jax import lax

WIDTH = 1280
HEADS = 20
TEXT_WIDTH = 2048
FREQS = 320
TEXT_TOKENS = 77
COLS = 32
ROWS = 4
MICRO = 4
STEPS = 2
N_SECTION = 4


def levels(stream_key, shape, split, low, largest):
    level = 1.0
    for axis_at, blocks in split:
        steps = jax.random.uniform(jax.random.fold_in(jax.random.fold_in(stream_key, 6), axis_at), (blocks,), jnp.float32, low / len(split), largest / len(split))
        level = level * jnp.repeat(jnp.exp(steps), shape[axis_at] // blocks).reshape((-1,) + (1,) * (len(shape) - 1 - axis_at))
    return level


def noise(key, shape, scale, most, shards=(), kind=jnp.bfloat16):
    drawn = jax.random.normal(key, shape, jnp.float32) * scale
    if len(shards) > 0:
        drawn = levels(key, shape, shards, -0.22, 0.18) * drawn
    return jnp.clip(drawn, min=-most, max=most).astype(kind)


def setup_inputs(seed: int = 0, part: int = 0) -> dict:
    seeds = jax.random.split(jax.random.key(seed), 13)
    own_keys = jax.random.split(jax.random.fold_in(seeds[12], part), 13)
    latents = noise(own_keys[0], (MICRO, ROWS, COLS, WIDTH), 1.0, 6.0, ((1, 4),))
    prompt_tokens = noise(own_keys[1], (MICRO, TEXT_TOKENS, TEXT_WIDTH), 1.0, 6.0)
    fresh_noise = noise(own_keys[2], (STEPS - 1, MICRO, ROWS, COLS, WIDTH), 1.0, 6.0, ((2, 4),))
    timesteps = jax.random.randint(seeds[3], (STEPS,), 600, 1000).astype(jnp.int32)
    entry_order = jax.random.permutation(own_keys[4], MICRO).astype(jnp.int32)
    timestep_weight = noise(seeds[5], (N_SECTION, FREQS, WIDTH), FREQS ** -0.5, 0.3125, ((0, 4),))
    conv_kernel = noise(seeds[6], (N_SECTION, 9, WIDTH), 0.2, 1.0, ((0, 4),), jnp.float32)
    norm_gain = jnp.clip(1.0 + 0.15 * jax.random.normal(seeds[7], (N_SECTION, WIDTH), jnp.float32), 0.25, 1.75)
    layer_norm_bias = noise(seeds[8], (N_SECTION, WIDTH), 0.3, 1.5, ((0, 4),), jnp.float32)
    qkv_weight = noise(seeds[9], (N_SECTION, WIDTH, 3, WIDTH), WIDTH ** -0.5, 0.15625, ((0, 4), (3, 4)))
    prompt_weight = noise(seeds[10], (N_SECTION, TEXT_WIDTH, 2, WIDTH), TEXT_WIDTH ** -0.5, 0.125, ((0, 4), (3, 4)))
    out_weight = noise(seeds[11], (N_SECTION, WIDTH, WIDTH), WIDTH ** -0.5, 0.15625, ((0, 4), (1, 4)))
    return dict(latents=latents, prompt_tokens=prompt_tokens, fresh_noise=fresh_noise, timesteps=timesteps, entry_order=entry_order, timestep_weight=timestep_weight, conv_kernel=conv_kernel, norm_gain=norm_gain, layer_norm_bias=layer_norm_bias, qkv_weight=qkv_weight, prompt_weight=prompt_weight, out_weight=out_weight)


def noise_plan():
    positions = jnp.arange(1000, dtype=jnp.float32)
    low_root = math.sqrt(0.00085)
    high_root = math.sqrt(0.012)
    roots = low_root + (high_root - low_root) * positions / 999.0
    return jnp.exp(jnp.cumsum(jnp.log(1.0 - roots * roots)))

def time_features(timesteps, half_count):
    exponents = jnp.arange(half_count, dtype=jnp.float32) / half_count
    freq_row = jnp.exp(-math.log(10000.0) * exponents)
    angles = timesteps.astype(jnp.float32)[:, None] * freq_row[None, :]
    return jnp.concatenate([jnp.cos(angles), jnp.sin(angles)], axis=1).astype(jnp.bfloat16)

def pick_scalar(alpha_table, position):
    hits = jnp.arange(alpha_table.shape[0], dtype=jnp.int32) == position
    return jnp.sum(jnp.where(hits, alpha_table, jnp.zeros_like(alpha_table)))

def mix_positions(rimmed, kernel_body):
    row_total = rimmed.shape[0] - 2
    col_total = rimmed.shape[1]
    framed = jnp.pad(rimmed.astype(jnp.float32), ((0, 0), (1, 1), (0, 0)))
    mixed = rimmed[1:-1].astype(jnp.float32)
    for offset_row in range(3):
        for offset_col in range(3):
            mixed = mixed + kernel_body[3 * offset_row + offset_col] * framed[offset_row:offset_row + row_total, offset_col:offset_col + col_total]
    return mixed

def layer_norm(values_in, scale_row, shift_row):
    centre = lax.optimization_barrier(jnp.mean(values_in, axis=-1, keepdims=True))
    spread = lax.optimization_barrier(jnp.mean(jnp.square(values_in - centre), axis=-1, keepdims=True))
    return (values_in - centre) * lax.rsqrt(spread + 1e-05) * scale_row + shift_row

def attention(queries, keys_all, values_all, head_count):
    query_count = queries.shape[0]
    key_count = keys_all.shape[0]
    head_width = queries.shape[1] // head_count
    query_heads = queries.astype(jnp.float32).reshape(query_count, head_count, head_width)
    key_heads = keys_all.astype(jnp.float32).reshape(key_count, head_count, head_width)
    value_heads = values_all.astype(jnp.float32).reshape(key_count, head_count, head_width)
    scores = jnp.einsum('qhd,khd->hqk', query_heads, key_heads) / math.sqrt(head_width)
    powers = jnp.exp(scores)
    soft_weights = (powers / lax.optimization_barrier(jnp.sum(powers, axis=-1, keepdims=True))).astype(jnp.bfloat16)
    attended = jnp.einsum('hqk,khd->qhd', soft_weights.astype(jnp.float32), value_heads)
    return attended.reshape(query_count, head_count * head_width).astype(jnp.bfloat16)

def run_section(current, temb_row, kernel_body, scale_row, shift_row, qkv_mat, prompt_mat, out_mat, prompt_row):
    rows_all, cols_all, width_all = current.shape
    lifted = (current.astype(jnp.float32) + temb_row).astype(jnp.bfloat16)
    rimmed = jnp.pad(lifted, ((1, 1), (0, 0), (0, 0)))
    mixed = mix_positions(rimmed, kernel_body).reshape(rows_all * cols_all, width_all)
    normed = layer_norm(mixed, scale_row, shift_row).astype(jnp.bfloat16)
    projected = jnp.einsum('tc,cjd->tjd', normed.astype(jnp.float32), qkv_mat.astype(jnp.float32)).astype(jnp.bfloat16)
    prompt_proj = jnp.einsum('tc,cjd->tjd', prompt_row.astype(jnp.float32), prompt_mat.astype(jnp.float32)).astype(jnp.bfloat16)
    keys_all = jnp.concatenate([projected[:, 1], prompt_proj[:, 0]], axis=0)
    values_all = jnp.concatenate([projected[:, 2], prompt_proj[:, 1]], axis=0)
    attended = attention(projected[:, 0], keys_all, values_all, HEADS)
    update = jnp.dot(attended, out_mat, preferred_element_type=jnp.float32)
    return (mixed + update).astype(jnp.bfloat16).reshape(rows_all, cols_all, width_all)

def reference(latents, prompt_tokens, fresh_noise, timesteps, entry_order, timestep_weight, conv_kernel, norm_gain, layer_norm_bias, qkv_weight, prompt_weight, out_weight):
    alpha_table = noise_plan()
    feature_rows = time_features(timesteps, timestep_weight.shape[1] // 2)
    timestep_embedding_all = jnp.einsum('zm,rmk->rzk', feature_rows.astype(jnp.float32), timestep_weight.astype(jnp.float32))
    results = jnp.zeros_like(latents)
    for slot_index in range(MICRO):
        latent_id = entry_order[slot_index].astype(jnp.int32)
        current = lax.dynamic_index_in_dim(latents, latent_id, 0, False)
        prompt_row = lax.dynamic_index_in_dim(prompt_tokens, latent_id, 0, False)
        for chain_level in range(STEPS):
            if chain_level > 0:
                alpha_bar = pick_scalar(alpha_table, timesteps[chain_level])
                current = (jnp.sqrt(alpha_bar) * current.astype(jnp.float32) + jnp.sqrt(1.0 - alpha_bar) * fresh_noise[chain_level - 1, slot_index].astype(jnp.float32)).astype(jnp.bfloat16)

            def section_step(state_now, section_inputs):
                temb_row, kernel_body, scale_row, shift_row, qkv_mat, prompt_mat, out_mat = section_inputs
                return (run_section(state_now, temb_row, kernel_body, scale_row, shift_row, qkv_mat, prompt_mat, out_mat, prompt_row), None)
            section_inputs = (timestep_embedding_all[:, chain_level], conv_kernel, norm_gain, layer_norm_bias, qkv_weight, prompt_weight, out_weight)
            scanned = lax.scan(section_step, current, section_inputs)
            current = scanned[0]
        results = results.at[latent_id].set(current)
    return results
```

```python
import functools
import math

import jax
import jax.numpy as jnp
from jax import lax
from jax.experimental import pallas as pl
from jax.experimental.pallas import tpu as pltpu
from jax.sharding import PartitionSpec as P

HEADS = 20
LANES = 128


def noise_plan():
    positions = jnp.arange(1000, dtype=jnp.float32)
    low_root = math.sqrt(0.00085)
    high_root = math.sqrt(0.012)
    roots = low_root + (high_root - low_root) * positions / 999.0
    return jnp.exp(jnp.cumsum(jnp.log(1.0 - roots * roots)))


def time_features(timesteps, half_count):
    exponents = jnp.arange(half_count, dtype=jnp.float32) / half_count
    freq_row = jnp.exp(-math.log(10000.0) * exponents)
    angles = timesteps.astype(jnp.float32)[:, None] * freq_row[None, :]
    return jnp.concatenate([jnp.cos(angles), jnp.sin(angles)], axis=1).astype(jnp.bfloat16)


def pick_scalar(alpha_table, position):
    hits = jnp.arange(alpha_table.shape[0], dtype=jnp.int32) == position
    return jnp.sum(jnp.where(hits, alpha_table, jnp.zeros_like(alpha_table)))


def swapped(value, axis, mask):
    count = lax.axis_size(axis)
    return lax.ppermute(value, axis, [(i, i ^ mask) for i in range(count)])


def prompt_kernel(token_ref, weight_ref, out_ref):
    slots = token_ref.shape[1]
    rows = lax.dot_general(
        weight_ref[...],
        token_ref[...].reshape(2 * slots, token_ref.shape[2]),
        (((1,), (1,)), ((), ())),
        preferred_element_type=jnp.float32,
    ).astype(jnp.bfloat16)
    out_ref[0] = rows[:, :slots]
    out_ref[1] = rows[:, slots:]


def project_prompts(tokens, weight):
    count, slots, width = tokens.shape
    rows = weight.shape[0]
    return pl.pallas_call(
        prompt_kernel,
        grid=(count // 2,),
        in_specs=[
            pl.BlockSpec((2, slots, width), lambda i: (i, 0, 0)),
            pl.BlockSpec((rows, width), lambda i: (0, 0)),
        ],
        out_specs=pl.BlockSpec((2, rows, slots), lambda i: (i, 0, 0)),
        out_shape=jax.ShapeDtypeStruct((count, rows, slots), jnp.bfloat16),
        compiler_params=pltpu.CompilerParams(vmem_limit_bytes=24 * 2**20),
        name="prompts",
    )(tokens, weight)


def stage_kernel(slot_parts, cols, head_width, token_total, renoise, *refs):
    flag_ref, mix_ref, x_ref = refs[:3]
    refs = refs[3:]
    if renoise:
        noise_ref, refs = refs[0], refs[1:]
    temb_ref, conv_ref, gain_ref, bias_ref, prompt_ref = refs[:5]
    refs = refs[5:]
    part_total = sum(2 if parts == 1 else 8 for parts in slot_parts)
    weight_refs, refs = refs[:part_total], refs[part_total:]
    out_ref, stored, sems, proj, mixed_ref, normed_ref, heads_ref = refs
    positions, width = x_ref.shape
    span = stored.shape[1] // len(slot_parts)
    half = span // 2
    chunk_total = width // LANES

    @pl.when(flag_ref[0] == 1)
    def _():
        parity = flag_ref[1]
        copies = [[] for _ in range(4)]
        at = 0
        for slot, parts in enumerate(slot_parts):
            for piece in range(4):
                if parts == 1:
                    source = weight_refs[at].at[piece] if piece < 3 else weight_refs[at + 1]
                    target = stored.at[piece, pl.ds(slot * span, span)]
                    copies[piece].append((source, target, sems.at[piece, 2 * slot]))
                else:
                    for second in range(2):
                        source = weight_refs[at + 4 * second + piece]
                        place = parity if second == 0 else 1 - parity
                        start = pl.multiple_of(slot * span + place * half, 16)
                        target = stored.at[piece, pl.ds(start, half)]
                        copies[piece].append((source, target, sems.at[piece, 2 * slot + second]))
            at += 2 if parts == 1 else 8
        copies = [[pltpu.make_async_copy(*c) for c in row] for row in copies]
        for row in copies:
            for copy in row:
                copy.start()

        place = lax.broadcasted_iota(jnp.int32, (positions, LANES), 0) % cols
        first = place == 0
        last = place == cols - 1
        gap = jnp.zeros((cols, LANES), jnp.float32)

        def mix_chunk(index, total):
            lanes = pl.ds(pl.multiple_of(index * LANES, LANES), LANES)
            value = x_ref[:, lanes].astype(jnp.float32)
            if renoise:
                value = mix_ref[0] * value + mix_ref[1] * noise_ref[:, lanes].astype(jnp.float32)
                value = value.astype(jnp.bfloat16).astype(jnp.float32)
            value = (value + temb_ref[:, lanes]).astype(jnp.bfloat16).astype(jnp.float32)
            before = jnp.where(first, 0.0, pltpu.roll(value, 1, 0))
            after = jnp.where(last, 0.0, pltpu.roll(value, positions - 1, 0))
            taps = conv_ref[:, lanes]

            def row_of(a):
                return (
                    taps[3 * a : 3 * a + 1] * before
                    + taps[3 * a + 1 : 3 * a + 2] * value
                    + taps[3 * a + 2 : 3 * a + 3] * after
                )

            mixed = value + row_of(1)
            mixed = mixed + jnp.concatenate([gap, row_of(0)[: positions - cols]], axis=0)
            mixed = mixed + jnp.concatenate([row_of(2)[cols:], gap], axis=0)
            mixed_ref[:, lanes] = mixed
            return total + mixed

        total = lax.fori_loop(
            0, chunk_total, mix_chunk, jnp.zeros((positions, LANES), jnp.float32)
        )
        centre = jnp.sum(total, axis=1, keepdims=True) / width

        def spread_chunk(index, total):
            lanes = pl.ds(pl.multiple_of(index * LANES, LANES), LANES)
            return total + jnp.square(mixed_ref[:, lanes] - centre)

        total = lax.fori_loop(
            0, chunk_total, spread_chunk, jnp.zeros((positions, LANES), jnp.float32), unroll=2
        )
        scale = lax.rsqrt(jnp.sum(total, axis=1, keepdims=True) / width + 1e-05)

        def norm_chunk(index, carry):
            lanes = pl.ds(pl.multiple_of(index * LANES, LANES), LANES)
            value = (mixed_ref[:, lanes] - centre) * scale
            normed_ref[:, lanes] = (value * gain_ref[:, lanes] + bias_ref[:, lanes]).astype(
                jnp.bfloat16
            )
            return carry

        lax.fori_loop(0, chunk_total, norm_chunk, 0, unroll=2)

        for piece in range(3):
            for copy in copies[piece]:
                copy.wait()
            for slot in range(0, len(slot_parts), 2):
                rows = pl.ds(slot * span, 2 * span)
                proj[piece, rows] = lax.dot_general(
                    stored[piece, rows],
                    normed_ref[...],
                    (((1,), (1,)), ((), ())),
                    preferred_element_type=jnp.float32,
                ).astype(jnp.bfloat16)

        prompt_slots = prompt_ref.shape[2]
        usable = lax.broadcasted_iota(jnp.int32, (prompt_slots, positions), 0) < token_total
        factor = 1.0 / math.sqrt(head_width)

        def head_result(row):
            rows = pl.ds(row, head_width)
            keys = jnp.concatenate([proj[1, rows], prompt_ref[0, rows]], axis=1)
            values = jnp.concatenate([proj[2, rows], prompt_ref[1, rows]], axis=1)
            scores = lax.dot_general(
                keys, proj[0, rows], (((0,), (0,)), ((), ())), preferred_element_type=jnp.float32
            )
            powers = jnp.exp(scores * factor)
            powers = jnp.concatenate(
                [powers[:positions], jnp.where(usable, powers[positions:], 0.0)], axis=0
            )
            soft = powers * (1.0 / jnp.sum(powers, axis=0, keepdims=True))
            return jnp.dot(values, soft.astype(jnp.bfloat16), preferred_element_type=jnp.float32)

        pair = 2 * head_width

        def pair_step(index, carry):
            row = pl.multiple_of(index * pair, pair)
            both = jnp.concatenate([head_result(row), head_result(row + head_width)], axis=0)
            heads_ref[:, pl.ds(row, pair)] = both.T.astype(jnp.bfloat16)
            return carry

        lax.fori_loop(0, stored.shape[1] // pair, pair_step, 0, unroll=2)

        for copy in copies[3]:
            copy.wait()
        piece = 2 * LANES
        for start in range(0, width, piece):
            lanes = pl.ds(start, piece)
            update = jnp.dot(heads_ref[...], stored[3, :, lanes], preferred_element_type=jnp.float32)
            out_ref[:, lanes] = (mixed_ref[:, lanes] + update).astype(jnp.bfloat16)


def run_stage(flags, mix, x, noise, temb, taps, gain, bias, prompts, slots, cols, head_width, tokens):
    positions, width = x.shape
    slot_parts = tuple(1 if len(slot) == 2 else 2 for slot in slots)
    weights = [piece for slot in slots for piece in slot]
    rows = prompts.shape[1]
    vmem = pl.BlockSpec(memory_space=pltpu.VMEM)
    smem = pl.BlockSpec(memory_space=pltpu.SMEM)
    hbm = pl.BlockSpec(memory_space=pltpu.HBM)
    inputs = [x] + ([noise] if noise is not None else []) + [temb, taps, gain, bias, prompts]
    return pl.pallas_call(
        functools.partial(
            stage_kernel, slot_parts, cols, head_width, tokens, noise is not None
        ),
        in_specs=[smem, smem] + [vmem] * len(inputs) + [hbm] * len(weights),
        out_specs=vmem,
        out_shape=jax.ShapeDtypeStruct((positions, width), jnp.bfloat16),
        scratch_shapes=[
            pltpu.VMEM((4, rows, width), jnp.bfloat16),
            pltpu.SemaphoreType.DMA((4, 2 * len(slots))),
            pltpu.VMEM((3, rows, positions), jnp.bfloat16),
            pltpu.VMEM((positions, width), jnp.float32),
            pltpu.VMEM((positions, width), jnp.bfloat16),
            pltpu.VMEM((positions, rows), jnp.bfloat16),
        ],
        compiler_params=pltpu.CompilerParams(vmem_limit_bytes=32 * 2**20),
        name="stage_noised" if noise is not None else "stage",
    )(flags, mix, *inputs, *weights)


def per_device(
    latents,
    prompt_tokens,
    fresh_noise,
    timesteps,
    entry_order,
    timestep_weight,
    conv_kernel,
    norm_gain,
    layer_norm_bias,
    qkv_weight,
    prompt_weight,
    out_weight,
):
    sections = lax.axis_size("section")
    tiles = lax.axis_size("tile")
    parts = lax.axis_size("batch")
    section = lax.axis_index("section")
    tile = lax.axis_index("tile")
    micro, rows_here, cols, width = latents.shape
    steps = timesteps.shape[0]
    head_width = width // HEADS
    span = qkv_weight.shape[3]
    tokens = prompt_tokens.shape[1]
    assert micro == tiles and tiles & (tiles - 1) == 0

    alpha_table = noise_plan()
    features = time_features(timesteps, timestep_weight.shape[1] // 2)
    temb = jnp.dot(features, timestep_weight[0], preferred_element_type=jnp.float32)

    own_qkv = qkv_weight[0].transpose(1, 2, 0)
    own_out = out_weight[0]
    half = span // 2
    paired = parts % 2 == 0
    parity = lax.axis_index("batch") % 2 if paired else jnp.int32(0)

    def own_half(which):
        taken = [lax.dynamic_slice_in_dim(own_qkv[i], which * half, half, 0) for i in range(3)]
        return taken + [lax.dynamic_slice_in_dim(own_out, which * half, half, 0)]

    def exchanged(source, axis, mask):
        return [swapped(piece, axis, mask) for piece in source]

    slots = [None] * tiles
    slots[0] = [own_qkv, own_out]
    bit = 1
    while bit < tiles:
        if bit == 1:
            slots[1] = exchanged(slots[0], "tile", 1)
        else:
            near = exchanged(own_half(parity), "tile", bit)
            if paired:
                far = exchanged(near, "batch", 1)
            else:
                far = exchanged(own_half(1), "tile", bit)
            slots[bit] = near + far
            for low in range(1, bit):
                slots[bit + low] = exchanged(slots[bit], "tile", low)
        bit *= 2

    def across(stack):
        mine = [lax.dynamic_index_in_dim(stack, tile ^ k, 0, False) for k in range(tiles)]
        return mine[:1] + [swapped(mine[k], "tile", k) for k in range(1, tiles)]

    def in_order(entries):
        stacked = jnp.stack(entries)
        return jnp.stack(
            [lax.dynamic_index_in_dim(stacked, tile ^ r, 0, False) for r in range(tiles)]
        )

    positions = tiles * rows_here * cols
    x = in_order(across(latents)).reshape(positions, width)

    padded = -(-tokens // LANES) * LANES
    token_rows = jnp.pad(prompt_tokens, ((0, 0), (0, padded - tokens), (0, 0)))
    prompt_rows = prompt_weight[0].transpose(1, 2, 0).reshape(2 * span, -1)
    prompt_local = project_prompts(token_rows, prompt_rows).reshape(micro, 2, span, padded)
    prompts = jnp.concatenate(across(prompt_local), axis=1)

    entry_of = jnp.sum(
        jnp.where(
            entry_order[None, :] == jnp.arange(micro, dtype=jnp.int32)[:, None],
            jnp.arange(micro, dtype=jnp.int32)[None, :],
            0,
        ),
        axis=1,
    )

    def noise_for(level):
        by_latent = jnp.take(fresh_noise[level - 1], entry_of, axis=0)
        return in_order(across(by_latent)).reshape(positions, width)

    taps = conv_kernel[0]
    for stage in range(steps * sections):
        level, group = divmod(stage, sections)
        noise = None
        mix = jnp.zeros((2,), jnp.float32)
        if level > 0 and group == 0:
            noise = noise_for(level)
            alpha_bar = pick_scalar(alpha_table, timesteps[level])
            mix = jnp.stack([jnp.sqrt(alpha_bar), jnp.sqrt(1.0 - alpha_bar)])
        flags = jnp.stack([(section == group).astype(jnp.int32), parity.astype(jnp.int32)])
        x = run_stage(
            flags, mix, x, noise, temb[level : level + 1], taps, norm_gain, layer_norm_bias,
            prompts, slots, cols, head_width, tokens,
        )
        if stage + 1 < steps * sections:
            x = lax.ppermute(x, "section", [(group, (group + 1) % sections)])

    share = width // sections
    final = sections - 1
    mine = x[:, final * share :]
    for other in range(final):
        piece = x[:, other * share : (other + 1) * share]
        mine = jnp.where(section == other, lax.ppermute(piece, "section", [(final, other)]), mine)
    blocks = mine.reshape(tiles, rows_here, cols, share)
    return in_order(across(blocks))


def solution(mesh):
    placed = (
        P("batch", "tile", None, None),
        P("batch", None, None),
        P(None, "batch", "tile", None, None),
        P(),
        P("batch"),
        P("section", None, None),
        P("section", None, None),
        P("section", None),
        P("section", None),
        P("section", None, None, "tile"),
        P("section", None, None, "tile"),
        P("section", "tile", None),
    )
    return jax.shard_map(
        per_device,
        mesh=mesh,
        in_specs=placed,
        out_specs=P("batch", "tile", None, "section"),
        check_vma=False,
    )
```

```python
import functools
import math

import jax
import jax.numpy as jnp
from jax import lax
from jax.experimental import pallas as pl
from jax.experimental.pallas import tpu as pltpu
from jax.sharding import PartitionSpec as P

HEADS = 20
LANES = 128


def noise_plan():
    positions = jnp.arange(1000, dtype=jnp.float32)
    low_root = math.sqrt(0.00085)
    high_root = math.sqrt(0.012)
    roots = low_root + (high_root - low_root) * positions / 999.0
    return jnp.exp(jnp.cumsum(jnp.log(1.0 - roots * roots)))


def time_features(timesteps, half_count):
    exponents = jnp.arange(half_count, dtype=jnp.float32) / half_count
    freq_row = jnp.exp(-math.log(10000.0) * exponents)
    angles = timesteps.astype(jnp.float32)[:, None] * freq_row[None, :]
    return jnp.concatenate([jnp.cos(angles), jnp.sin(angles)], axis=1).astype(jnp.bfloat16)


def pick_scalar(alpha_table, position):
    hits = jnp.arange(alpha_table.shape[0], dtype=jnp.int32) == position
    return jnp.sum(jnp.where(hits, alpha_table, jnp.zeros_like(alpha_table)))


def swapped(value, axis, mask):
    count = lax.axis_size(axis)
    return lax.ppermute(value, axis, [(i, i ^ mask) for i in range(count)])


def prompt_kernel(token_ref, weight_ref, out_ref):
    slots = token_ref.shape[1]
    rows = lax.dot_general(
        weight_ref[...],
        token_ref[...].reshape(2 * slots, token_ref.shape[2]),
        (((1,), (1,)), ((), ())),
        preferred_element_type=jnp.float32,
    ).astype(jnp.bfloat16)
    out_ref[0] = rows[:, :slots]
    out_ref[1] = rows[:, slots:]


def project_prompts(tokens, weight):
    count, slots, width = tokens.shape
    rows = weight.shape[0]
    return pl.pallas_call(
        prompt_kernel,
        grid=(count // 2,),
        in_specs=[
            pl.BlockSpec((2, slots, width), lambda i: (i, 0, 0)),
            pl.BlockSpec((rows, width), lambda i: (0, 0)),
        ],
        out_specs=pl.BlockSpec((2, rows, slots), lambda i: (i, 0, 0)),
        out_shape=jax.ShapeDtypeStruct((count, rows, slots), jnp.bfloat16),
        compiler_params=pltpu.CompilerParams(vmem_limit_bytes=24 * 2**20),
        name="prompts",
    )(tokens, weight)


def cut_kernel(flag_ref, qkv_ref, last_ref, *refs):
    outs, sems = refs[:-1], refs[-1]
    half = outs[0].shape[0]
    rows = pl.ds(pl.multiple_of(flag_ref[0] * half, 16), half)
    copies = []
    for piece, out in enumerate(outs):
        source = qkv_ref.at[piece, rows] if piece < 3 else last_ref.at[rows]
        copies.append(pltpu.make_async_copy(source, out, sems.at[piece]))
    for copy in copies:
        copy.start()
    for copy in copies:
        copy.wait()


def cut(which, qkv, last):
    span, width = last.shape
    hbm = pl.BlockSpec(memory_space=pltpu.HBM)
    return pl.pallas_call(
        cut_kernel,
        in_specs=[pl.BlockSpec(memory_space=pltpu.SMEM), hbm, hbm],
        out_specs=[pl.BlockSpec(memory_space=pltpu.VMEM)] * 4,
        out_shape=[jax.ShapeDtypeStruct((span // 2, width), jnp.bfloat16)] * 4,
        scratch_shapes=[pltpu.SemaphoreType.DMA((4,))],
        compiler_params=pltpu.CompilerParams(vmem_limit_bytes=16 * 2**20),
        name="cut",
    )(which.reshape(1), qkv, last)


def assemble_kernel(counts, piece_total, flag_ref, *refs):
    total = sum(counts)
    sources, weight_ref, sems = refs[:total], refs[total], refs[total + 1]
    span = weight_ref.shape[1] // len(counts)
    parity = flag_ref[0]
    copies = []
    at = 0
    for slot, count in enumerate(counts):
        if count == 1:
            rows = pl.ds(slot * span, span)
            copies.append((sources[at], weight_ref.at[:, rows], sems.at[at]))
        else:
            for part in range(count):
                half = span // 2
                place = parity if part < piece_total else 1 - parity
                rows = pl.ds(pl.multiple_of(slot * span + place * half, 16), half)
                copies.append((sources[at + part], weight_ref.at[part % piece_total, rows], sems.at[at + part]))
        at += count
    copies = [pltpu.make_async_copy(*c) for c in copies]
    for copy in copies:
        copy.start()
    for copy in copies:
        copy.wait()


def assemble(parity, slots, name):
    piece_total, span, width = slots[0][0].shape
    sources = [piece for slot in slots for piece in slot]
    hbm = pl.BlockSpec(memory_space=pltpu.HBM)
    return pl.pallas_call(
        functools.partial(assemble_kernel, tuple(len(slot) for slot in slots), piece_total),
        in_specs=[pl.BlockSpec(memory_space=pltpu.SMEM)] + [hbm] * len(sources),
        out_specs=pl.BlockSpec(memory_space=pltpu.VMEM),
        out_shape=jax.ShapeDtypeStruct((piece_total, span * len(slots), width), jnp.bfloat16),
        scratch_shapes=[pltpu.SemaphoreType.DMA((len(sources),))],
        compiler_params=pltpu.CompilerParams(vmem_limit_bytes=16 * 2**20),
        name=name,
    )(parity.reshape(1), *sources)


def stage_kernel(cols, head_width, token_total, tiles, split, noised, *refs):
    flag_ref, mix_ref = refs[:2]
    refs = refs[2:]
    count = tiles if split else 1
    x_refs, refs = refs[:count], refs[count:]
    noise_refs, refs = (refs[:tiles], refs[tiles:]) if noised else (None, refs)
    temb_ref, conv_ref, gain_ref, bias_ref, prompt_ref, weight_ref, last_ref = refs[:7]
    out_ref, proj, mixed_ref, normed_ref, heads_ref, x_ref, noise_ref = refs[7:]
    positions, width = out_ref.shape
    rows_total = weight_ref.shape[1]
    block = positions // tiles
    chunk_total = width // LANES

    @pl.when(flag_ref[0] == 1)
    def _():
        tile = flag_ref[1]
        for k in range(tiles):
            rows = pl.ds(pl.multiple_of((tile ^ k) * block, 16), block)
            if split:
                x_ref[rows] = x_refs[k][...]
            if noised:
                noise_ref[rows] = noise_refs[k][...]
        source = x_ref if split else x_refs[0]

        place = lax.broadcasted_iota(jnp.int32, (positions, LANES), 0) % cols
        first = place == 0
        last = place == cols - 1
        gap = jnp.zeros((cols, LANES), jnp.float32)

        def mix_chunk(index, total):
            lanes = pl.ds(pl.multiple_of(index * LANES, LANES), LANES)
            value = source[:, lanes].astype(jnp.float32)
            if noised:
                value = mix_ref[0] * value + mix_ref[1] * noise_ref[:, lanes].astype(jnp.float32)
                value = value.astype(jnp.bfloat16).astype(jnp.float32)
            value = (value + temb_ref[:, lanes]).astype(jnp.bfloat16).astype(jnp.float32)
            before = jnp.where(first, 0.0, pltpu.roll(value, 1, 0))
            after = jnp.where(last, 0.0, pltpu.roll(value, positions - 1, 0))
            taps = conv_ref[:, lanes]

            def row_of(a):
                return (
                    taps[3 * a : 3 * a + 1] * before
                    + taps[3 * a + 1 : 3 * a + 2] * value
                    + taps[3 * a + 2 : 3 * a + 3] * after
                )

            mixed = value + row_of(1)
            mixed = mixed + jnp.concatenate([gap, row_of(0)[: positions - cols]], axis=0)
            mixed = mixed + jnp.concatenate([row_of(2)[cols:], gap], axis=0)
            mixed_ref[:, lanes] = mixed
            return total + mixed

        total = lax.fori_loop(
            0, chunk_total, mix_chunk, jnp.zeros((positions, LANES), jnp.float32)
        )
        centre = jnp.sum(total, axis=1, keepdims=True) / width

        def spread_chunk(index, total):
            lanes = pl.ds(pl.multiple_of(index * LANES, LANES), LANES)
            return total + jnp.square(mixed_ref[:, lanes] - centre)

        total = lax.fori_loop(
            0, chunk_total, spread_chunk, jnp.zeros((positions, LANES), jnp.float32), unroll=2
        )
        scale = lax.rsqrt(jnp.sum(total, axis=1, keepdims=True) / width + 1e-05)

        def norm_chunk(index, carry):
            lanes = pl.ds(pl.multiple_of(index * LANES, LANES), LANES)
            value = (mixed_ref[:, lanes] - centre) * scale
            normed_ref[:, lanes] = (value * gain_ref[:, lanes] + bias_ref[:, lanes]).astype(
                jnp.bfloat16
            )
            return carry

        lax.fori_loop(0, chunk_total, norm_chunk, 0, unroll=2)

        big = rows_total // 2
        for piece in range(3):
            for start in range(0, rows_total, big):
                rows = pl.ds(start, big)
                proj[piece, rows] = lax.dot_general(
                    weight_ref[piece, rows],
                    normed_ref[...],
                    (((1,), (1,)), ((), ())),
                    preferred_element_type=jnp.float32,
                ).astype(jnp.bfloat16)

        prompt_slots = prompt_ref.shape[2]
        pair = 2 * head_width
        usable = lax.broadcasted_iota(jnp.int32, (2 * positions, prompt_slots), 1) < token_total
        upper = lax.broadcasted_iota(jnp.int32, (positions, pair), 1) < head_width
        factor = 1.0 / math.sqrt(head_width)

        def pair_step(index, carry):
            rows = pl.ds(pl.multiple_of(index * pair, pair), pair)
            both = proj[0, rows].T
            nothing = jnp.zeros_like(both)
            queries = jnp.concatenate(
                [jnp.where(upper, both, nothing), jnp.where(upper, nothing, both)], axis=0
            )
            keys = jnp.concatenate([proj[1, rows], prompt_ref[0, rows]], axis=1)
            values = jnp.concatenate([proj[2, rows], prompt_ref[1, rows]], axis=1)
            scores = jnp.dot(queries, keys, preferred_element_type=jnp.float32)
            powers = jnp.exp(scores * factor)
            front = powers[:, :positions]
            rear = jnp.where(usable, powers[:, positions:], 0.0)
            if front.shape == rear.shape:
                whole = jnp.sum(front + rear, axis=1, keepdims=True)
            else:
                whole = jnp.sum(front, axis=1, keepdims=True) + jnp.sum(rear, axis=1, keepdims=True)
            inverse = 1.0 / whole
            soft = jnp.concatenate([front * inverse, rear * inverse], axis=1).astype(jnp.bfloat16)
            joined = lax.dot_general(
                soft, values, (((1,), (1,)), ((), ())), preferred_element_type=jnp.float32
            )
            heads_ref[:, rows] = jnp.where(upper, joined[:positions], joined[positions:]).astype(
                jnp.bfloat16
            )
            return carry

        lax.fori_loop(0, rows_total // pair, pair_step, 0, unroll=5)

        piece = 2 * LANES
        for start in range(0, width, piece):
            lanes = pl.ds(start, piece)
            update = jnp.dot(
                heads_ref[...], last_ref[0, :, lanes], preferred_element_type=jnp.float32
            )
            out_ref[:, lanes] = (mixed_ref[:, lanes] + update).astype(jnp.bfloat16)


def run_stage(flags, mix, x, noise, temb, taps, gain, bias, prompts, weights, last, cols, head_width, tokens, tiles):
    split = isinstance(x, list)
    noised = noise is not None
    width = weights.shape[2]
    positions = tiles * x[0].shape[0] if split else x.shape[0]
    rows = weights.shape[1]
    vmem = pl.BlockSpec(memory_space=pltpu.VMEM)
    smem = pl.BlockSpec(memory_space=pltpu.SMEM)
    inputs = (x if split else [x]) + (noise if noised else [])
    inputs = inputs + [temb, taps, gain, bias, prompts, weights, last]
    spare = (positions, width)
    return pl.pallas_call(
        functools.partial(stage_kernel, cols, head_width, tokens, tiles, split, noised),
        in_specs=[smem, smem] + [vmem] * len(inputs),
        out_specs=vmem,
        out_shape=jax.ShapeDtypeStruct((positions, width), jnp.bfloat16),
        scratch_shapes=[
            pltpu.VMEM((3, rows, positions), jnp.bfloat16),
            pltpu.VMEM((positions, width), jnp.float32),
            pltpu.VMEM((positions, width), jnp.bfloat16),
            pltpu.VMEM((positions, rows), jnp.bfloat16),
            pltpu.VMEM(spare if split else (16, LANES), jnp.bfloat16),
            pltpu.VMEM(spare if noised else (16, LANES), jnp.bfloat16),
        ],
        compiler_params=pltpu.CompilerParams(vmem_limit_bytes=24 * 2**20),
        name="stage_noised" if noised else "stage_first" if split else "stage",
    )(flags, mix, *inputs)


def per_device(
    latents,
    prompt_tokens,
    fresh_noise,
    timesteps,
    entry_order,
    timestep_weight,
    conv_kernel,
    norm_gain,
    layer_norm_bias,
    qkv_weight,
    prompt_weight,
    out_weight,
):
    sections = lax.axis_size("section")
    tiles = lax.axis_size("tile")
    parts = lax.axis_size("batch")
    section = lax.axis_index("section")
    tile = lax.axis_index("tile")
    micro, rows_here, cols, width = latents.shape
    steps = timesteps.shape[0]
    head_width = width // HEADS
    span = qkv_weight.shape[3]
    tokens = prompt_tokens.shape[1]
    assert micro == tiles and tiles & (tiles - 1) == 0

    alpha_table = noise_plan()
    features = time_features(timesteps, timestep_weight.shape[1] // 2)
    temb = jnp.dot(features, timestep_weight[0], preferred_element_type=jnp.float32)

    own_qkv = qkv_weight[0].transpose(1, 2, 0)
    own_out = out_weight[0]
    half = span // 2
    paired = parts % 2 == 0
    parity = lax.axis_index("batch") % 2 if paired else jnp.int32(0)
    parity = parity.astype(jnp.int32)

    def exchanged(source, axis, mask):
        return [swapped(piece, axis, mask) for piece in source]

    halves = list(cut(parity, own_qkv, own_out))
    halves, own_qkv, own_out, prompt_tokens, latents, fresh_noise = lax.optimization_barrier(
        (halves, own_qkv, own_out, prompt_tokens, latents, fresh_noise)
    )
    def picked(stack):
        return [lax.dynamic_index_in_dim(stack, tile ^ k, 0, False) for k in range(tiles)]

    def sent(mine, group=None):
        if group is None:
            return mine[:1] + [swapped(mine[k], "tile", k) for k in range(1, tiles)]
        first = group * tiles
        return mine[:1] + [
            lax.ppermute(
                mine[k], ("section", "tile"), [(first + t, first + (t ^ k)) for t in range(tiles)]
            )
            for k in range(1, tiles)
        ]

    def across(stack, group=None):
        return sent(picked(stack), group)

    def in_order(entries):
        stacked = jnp.stack(entries)
        return jnp.stack(
            [lax.dynamic_index_in_dim(stacked, tile ^ r, 0, False) for r in range(tiles)]
        )

    padded = -(-tokens // LANES) * LANES
    prompt_rows = prompt_weight[0].transpose(1, 2, 0).reshape(2 * span, -1)

    def relayed(near, early):
        if not paired:
            return exchanged(list(cut(1 - parity, own_qkv, own_out)), "tile", bit) + [early]
        far = []
        for piece in range(4):
            if piece == 1:
                near[1], early = lax.optimization_barrier((near[1], early))
            if piece > 1:
                near[piece], far[piece - 2] = lax.optimization_barrier((near[piece], far[piece - 2]))
            if piece == 2:
                near[2], early = lax.optimization_barrier((near[2], early))
            far.append(swapped(near[piece], "batch", 1))
        return far + [early]

    slots = [None] * tiles
    slots[0] = [own_qkv, own_out[None]]
    x = prompts = None
    bit = 1
    while bit < tiles:
        if bit == 1:
            slots[1] = exchanged(slots[0], "tile", 1)
        else:
            near = exchanged(halves, "tile", bit)
            if prompts is None:
                token_rows = jnp.pad(prompt_tokens, ((0, 0), (0, padded - tokens), (0, 0)))
                prompt_local = project_prompts(token_rows, prompt_rows)
                prompt_local = prompt_local.reshape(micro, 2, span, padded)
                mine, first = picked(prompt_local), picked(latents)
                far = relayed(near, [mine, first])
                mine, first = far.pop()
                prompts, x = sent(mine), sent(first, 0)
                far[3], prompts, x = lax.optimization_barrier((far[3], prompts, x))
            else:
                far = relayed(near, [])[:4]
            slots[bit] = near + far
            for low in range(1, bit):
                slots[bit + low] = exchanged(slots[bit], "tile", low)
        bit *= 2
    prompts = [[piece] for piece in prompts]
    x = [piece.reshape(rows_here * cols, width) for piece in x]

    entry_of = jnp.sum(
        jnp.where(
            entry_order[None, :] == jnp.arange(micro, dtype=jnp.int32)[:, None],
            jnp.arange(micro, dtype=jnp.int32)[None, :],
            0,
        ),
        axis=1,
    )
    noises = [None]
    mixes = [jnp.zeros((2,), jnp.float32)]
    for level in range(1, steps):
        by_latent = jnp.take(fresh_noise[level - 1], entry_of, axis=0)
        noises.append([n.reshape(rows_here * cols, width) for n in picked(by_latent)])
        alpha_bar = pick_scalar(alpha_table, timesteps[level])
        mixes.append(jnp.stack([jnp.sqrt(alpha_bar), jnp.sqrt(1.0 - alpha_bar)]))
    flags = [
        jnp.stack([(section == group).astype(jnp.int32), tile.astype(jnp.int32)])
        for group in range(sections)
    ]
    tembs = [temb[level : level + 1] for level in range(steps)]
    taps = conv_kernel[0]
    firsts = [slot[:1] if len(slot) == 2 else slot[:3] + slot[4:7] for slot in slots]
    lasts = [slot[1:] if len(slot) == 2 else slot[3:4] + slot[7:] for slot in slots]
    firsts, prompts, mixes, flags, tembs, taps, noises = lax.optimization_barrier(
        (firsts, prompts, mixes, flags, tembs, taps, noises)
    )
    prompts = assemble(parity, prompts, "prompts_in")
    weights = assemble(parity, firsts, "weights_in")
    last = assemble(parity, lasts, "last_in")
    noises = [None] + [sent(mine, 0) for mine in noises[1:]]

    for stage in range(steps * sections):
        level, group = divmod(stage, sections)
        noise = noises[level] if group == 0 else None
        x = run_stage(
            flags[group], mixes[level], x, noise, tembs[level], taps, norm_gain, layer_norm_bias,
            prompts, weights, last, cols, head_width, tokens, tiles,
        )
        if stage + 1 < steps * sections:
            x = lax.ppermute(x, "section", [(group, (group + 1) % sections)])

    share = width // sections
    final = sections - 1
    mine = x[:, final * share :]
    for other in range(final):
        piece = x[:, other * share : (other + 1) * share]
        mine = jnp.where(section == other, lax.ppermute(piece, "section", [(final, other)]), mine)
    blocks = mine.reshape(tiles, rows_here, cols, share)
    return in_order(across(blocks))


def solution(mesh):
    placed = (
        P("batch", "tile", None, None),
        P("batch", None, None),
        P(None, "batch", "tile", None, None),
        P(),
        P("batch"),
        P("section", None, None),
        P("section", None, None),
        P("section", None),
        P("section", None),
        P("section", None, None, "tile"),
        P("section", None, None, "tile"),
        P("section", "tile", None),
    )
    return jax.shard_map(
        per_device,
        mesh=mesh,
        in_specs=placed,
        out_specs=P("batch", "tile", None, "section"),
        check_vma=False,
    )
```

```python
import functools
import math

import jax
import jax.numpy as jnp
from jax import lax
from jax.experimental import pallas as pl
from jax.experimental.pallas import tpu as pltpu
from jax.sharding import PartitionSpec as P


HEADS = 20
LANES = 128


def alpha_bar_at(position):
    shape = (8, LANES)
    positions = lax.broadcasted_iota(jnp.int32, shape, 0) * LANES
    positions = positions + lax.broadcasted_iota(jnp.int32, shape, 1)
    low_root = math.sqrt(0.00085)
    high_root = math.sqrt(0.012)
    roots = low_root + (high_root - low_root) * positions.astype(jnp.float32) / 999.0
    logs = jnp.where(positions <= position, jnp.log(1.0 - roots * roots), 0.0)
    return jnp.exp(jnp.sum(jnp.sum(logs, axis=1, keepdims=True), axis=0, keepdims=True))


def time_features(timesteps, half_count):
    exponents = jnp.arange(half_count, dtype=jnp.float32) / half_count
    freq_row = jnp.exp(-math.log(10000.0) * exponents)
    angles = timesteps.astype(jnp.float32)[:, None] * freq_row[None, :]
    return jnp.concatenate([jnp.cos(angles), jnp.sin(angles)], axis=1).astype(jnp.bfloat16)


def swapped(value, axis, mask):
    count = lax.axis_size(axis)
    return lax.ppermute(value, axis, [(i, i ^ mask) for i in range(count)])


def prompt_kernel(token_ref, weight_ref, out_ref):
    slots = token_ref.shape[1]
    rows = lax.dot_general(
        weight_ref[...],
        token_ref[...].reshape(2 * slots, token_ref.shape[2]),
        (((1,), (1,)), ((), ())),
        preferred_element_type=jnp.float32,
    ).astype(jnp.bfloat16)
    out_ref[0] = rows[:, :slots]
    out_ref[1] = rows[:, slots:]


def project_prompts(tokens, weight):
    count, slots, width = tokens.shape
    rows = weight.shape[0]
    return pl.pallas_call(
        prompt_kernel,
        grid=(count // 2,),
        in_specs=[
            pl.BlockSpec((2, slots, width), lambda i: (i, 0, 0)),
            pl.BlockSpec((rows, width), lambda i: (0, 0)),
        ],
        out_specs=pl.BlockSpec((2, rows, slots), lambda i: (i, 0, 0)),
        out_shape=jax.ShapeDtypeStruct((count, rows, slots), jnp.bfloat16),
        compiler_params=pltpu.CompilerParams(vmem_limit_bytes=60 * 2**20),
        name="prompts",
    )(tokens, weight)


def pick_kernel(masks, block, flag_ref, order_ref, source_ref, *refs):
    outs, sems = refs[:-1], refs[-1]
    tile = flag_ref[1]
    copies = []
    for index, out in enumerate(outs):
        for j, mask in enumerate(masks[index]):
            entry = tile ^ mask
            if order_ref is not None:
                wanted = entry
                entry = jnp.int32(0)
                for m in range(order_ref.shape[0]):
                    entry = entry + jnp.where(order_ref[m] == wanted, m, 0)
            rows = pl.ds(pl.multiple_of(entry * block, 16), block)
            copies.append(
                pltpu.make_async_copy(source_ref.at[rows], out.at[j], sems.at[index, j])
            )
    for copy in copies:
        copy.start()
    for copy in copies:
        copy.wait()


def pick(flags, order, source, block, masks, vmem_total):
    kernel = functools.partial(pick_kernel, masks, block)
    if order is None:
        kernel = lambda flag_ref, *refs: pick_kernel(masks, block, flag_ref, None, *refs)
    smem = pl.BlockSpec(memory_space=pltpu.SMEM)
    width = source.shape[1]
    return pl.pallas_call(
        kernel,
        in_specs=[smem] + ([smem] if order is not None else []) + [pl.BlockSpec(memory_space=pltpu.HBM)],
        out_specs=[pl.BlockSpec(memory_space=pltpu.VMEM)] * len(masks),
        out_shape=[jax.ShapeDtypeStruct((len(m), block, width), source.dtype) for m in masks],
        scratch_shapes=[pltpu.SemaphoreType.DMA((len(masks), len(masks[0])))],
        compiler_params=pltpu.CompilerParams(vmem_limit_bytes=vmem_total * 2**20),
    )(flags, *([order] if order is not None else []), source)


def cut_kernel(which, flag_ref, qkv_ref, last_ref, *refs):
    outs, sems = refs[:-1], refs[-1]
    half = outs[0].shape[0]
    parity = flag_ref[2] if which == 0 else 1 - flag_ref[2]
    rows = pl.ds(pl.multiple_of(parity * half, 16), half)
    copies = []
    for piece, out in enumerate(outs):
        source = qkv_ref.at[piece, rows] if piece < 3 else last_ref.at[rows]
        copies.append(pltpu.make_async_copy(source, out, sems.at[piece]))
    for copy in copies:
        copy.start()
    for copy in copies:
        copy.wait()


def cut(flags, which, qkv, last):
    span, width = last.shape
    hbm = pl.BlockSpec(memory_space=pltpu.HBM)
    return pl.pallas_call(
        functools.partial(cut_kernel, which),
        in_specs=[pl.BlockSpec(memory_space=pltpu.SMEM), hbm, hbm],
        out_specs=[pl.BlockSpec(memory_space=pltpu.VMEM)] * 4,
        out_shape=[jax.ShapeDtypeStruct((span // 2, width), jnp.bfloat16)] * 4,
        scratch_shapes=[pltpu.SemaphoreType.DMA((4,))],
        compiler_params=pltpu.CompilerParams(vmem_limit_bytes=60 * 2**20),
        name="cut",
    )(flags, qkv, last)


def assemble_kernel(layouts, group, flag_ref, *refs):
    total = sum(sum(counts) for counts, _ in layouts)
    sources, outs, sems = refs[:total], refs[total:-1], refs[-1]
    parity = flag_ref[2]
    copies = []
    at = 0
    for out, (counts, piece_total) in zip(outs, layouts):
        span = out.shape[1] // len(counts)
        for slot, count in enumerate(counts):
            for part in range(count):
                source, sem = sources[at], sems.at[at]
                at += 1
                if count == 1:
                    target = out.at[:, pl.ds(slot * span, span)]
                else:
                    half = span // 2
                    place = parity if part < piece_total else 1 - parity
                    rows = pl.ds(pl.multiple_of(slot * span + place * half, 16), half)
                    target = out.at[part % piece_total, rows]
                copies.append(pltpu.make_async_copy(source, target, sem))

    @pl.when(flag_ref[0] == group if group is not None else flag_ref[0] >= 0)
    def _():
        for copy in copies:
            copy.start()
        for copy in copies:
            copy.wait()


def assemble(flags, group, arrays):
    layouts, sources, shapes = [], [], []
    for slots in arrays:
        piece_total, span, width = slots[0][0].shape
        layouts.append((tuple(len(slot) for slot in slots), piece_total))
        sources += [piece for slot in slots for piece in slot]
        shapes.append(jax.ShapeDtypeStruct((piece_total, span * len(slots), width), jnp.bfloat16))
    hbm = pl.BlockSpec(memory_space=pltpu.HBM)
    return pl.pallas_call(
        functools.partial(assemble_kernel, tuple(layouts), group),
        in_specs=[pl.BlockSpec(memory_space=pltpu.SMEM)] + [hbm] * len(sources),
        out_specs=[pl.BlockSpec(memory_space=pltpu.VMEM)] * len(shapes),
        out_shape=shapes,
        scratch_shapes=[pltpu.SemaphoreType.DMA((len(sources),))],
        compiler_params=pltpu.CompilerParams(vmem_limit_bytes=16 * 2**20),
    )(flags, *sources)


def stage_kernel(cols, head_width, token_total, tiles, count, mode, level, group, partial, *refs):
    noised = level > 0
    flag_ref, steps_ref = refs[:2]
    refs = refs[2:]
    x_refs, refs = refs[:count], refs[count:]
    noise_refs, refs = (refs[:tiles], refs[tiles:]) if noised else (None, refs)
    temb_ref, conv_ref, gain_ref, bias_ref, prompt_ref, weight_ref, last_ref = refs[:7]
    out_refs, refs = refs[7:-6], refs[-6:]
    proj, mixed_ref, normed_ref, heads_ref, x_ref, noise_ref = refs
    positions, width = mixed_ref.shape
    rows_total = weight_ref.shape[1]
    block = positions // tiles
    chunk_total = width // LANES

    @pl.when(flag_ref[0] == group)
    def _():
        tile = flag_ref[1]
        for k in range(tiles):
            rows = pl.ds(pl.multiple_of((tile ^ k) * block, 16), block)
            if mode in (0, 1):
                x_ref[rows] = x_refs[k][mode]
            if noised:
                noise_ref[rows] = noise_refs[k][0]
        sources = [x_ref] if mode in (0, 1) else x_refs

        if noised:
            alpha_bar = alpha_bar_at(steps_ref[level])
            keep, renew = jnp.sqrt(alpha_bar), jnp.sqrt(1.0 - alpha_bar)
        place = lax.broadcasted_iota(jnp.int32, (positions, LANES), 0) % cols
        first = place == 0
        last = place == cols - 1
        gap = jnp.zeros((cols, LANES), jnp.float32)

        def mix_chunk(index, total):
            lanes = pl.ds(pl.multiple_of(index * LANES, LANES), LANES)
            value = sources[0][:, lanes].astype(jnp.float32)
            for other in sources[1:]:
                value = (value + other[:, lanes].astype(jnp.float32)).astype(jnp.bfloat16)
                value = value.astype(jnp.float32)
            if noised:
                value = keep * value + renew * noise_ref[:, lanes].astype(jnp.float32)
                value = value.astype(jnp.bfloat16).astype(jnp.float32)
            value = (value + temb_ref[:, lanes]).astype(jnp.bfloat16).astype(jnp.float32)
            before = jnp.where(first, 0.0, pltpu.roll(value, 1, 0))
            after = jnp.where(last, 0.0, pltpu.roll(value, positions - 1, 0))
            taps = conv_ref[:, lanes]

            def row_of(a):
                return (
                    taps[3 * a : 3 * a + 1] * before
                    + taps[3 * a + 1 : 3 * a + 2] * value
                    + taps[3 * a + 2 : 3 * a + 3] * after
                )

            mixed = value + row_of(1)
            mixed = mixed + jnp.concatenate([gap, row_of(0)[: positions - cols]], axis=0)
            mixed = mixed + jnp.concatenate([row_of(2)[cols:], gap], axis=0)
            mixed_ref[:, lanes] = mixed
            return total + mixed

        total = lax.fori_loop(
            0, chunk_total, mix_chunk, jnp.zeros((positions, LANES), jnp.float32)
        )
        centre = jnp.sum(total, axis=1, keepdims=True) / width

        def spread_chunk(index, total):
            lanes = pl.ds(pl.multiple_of(index * LANES, LANES), LANES)
            return total + jnp.square(mixed_ref[:, lanes] - centre)

        total = lax.fori_loop(
            0, chunk_total, spread_chunk, jnp.zeros((positions, LANES), jnp.float32), unroll=2
        )
        scale = lax.rsqrt(jnp.sum(total, axis=1, keepdims=True) / width + 1e-05)

        def norm_chunk(index, carry):
            lanes = pl.ds(pl.multiple_of(index * LANES, LANES), LANES)
            value = (mixed_ref[:, lanes] - centre) * scale
            normed_ref[:, lanes] = (value * gain_ref[:, lanes] + bias_ref[:, lanes]).astype(
                jnp.bfloat16
            )
            return carry

        lax.fori_loop(0, chunk_total, norm_chunk, 0, unroll=2)

        big = rows_total // 2
        for piece in range(3):
            for start in range(0, rows_total, big):
                rows = pl.ds(start, big)
                proj[piece, rows] = lax.dot_general(
                    weight_ref[piece, rows],
                    normed_ref[...],
                    (((1,), (1,)), ((), ())),
                    preferred_element_type=jnp.float32,
                ).astype(jnp.bfloat16)

        prompt_slots = prompt_ref.shape[2]
        pair = 2 * head_width
        usable = lax.broadcasted_iota(jnp.int32, (2 * positions, prompt_slots), 1) < token_total
        upper = lax.broadcasted_iota(jnp.int32, (positions, pair), 1) < head_width
        factor = 1.0 / math.sqrt(head_width)

        def pair_step(index, carry):
            rows = pl.ds(pl.multiple_of(index * pair, pair), pair)
            both = proj[0, rows].T
            nothing = jnp.zeros_like(both)
            queries = jnp.concatenate(
                [jnp.where(upper, both, nothing), jnp.where(upper, nothing, both)], axis=0
            )
            keys = jnp.concatenate([proj[1, rows], prompt_ref[0, rows]], axis=1)
            values = jnp.concatenate([proj[2, rows], prompt_ref[1, rows]], axis=1)
            scores = jnp.dot(queries, keys, preferred_element_type=jnp.float32)
            powers = jnp.exp(scores * factor)
            front = powers[:, :positions]
            rear = jnp.where(usable, powers[:, positions:], 0.0)
            if front.shape == rear.shape:
                whole = jnp.sum(front + rear, axis=1, keepdims=True)
            else:
                whole = jnp.sum(front, axis=1, keepdims=True) + jnp.sum(rear, axis=1, keepdims=True)
            inverse = 1.0 / whole
            soft = jnp.concatenate([front * inverse, rear * inverse], axis=1).astype(jnp.bfloat16)
            joined = lax.dot_general(
                soft, values, (((1,), (1,)), ((), ())), preferred_element_type=jnp.float32
            )
            heads_ref[:, rows] = jnp.where(upper, joined[:positions], joined[positions:]).astype(
                jnp.bfloat16
            )
            return carry

        lax.fori_loop(0, rows_total // pair, pair_step, 0, unroll=5)

        piece = 2 * LANES
        for start in range(0, width, piece):
            lanes = pl.ds(start, piece)
            update = jnp.dot(
                heads_ref[...], last_ref[0, :, lanes], preferred_element_type=jnp.float32
            )
            final = update if partial else mixed_ref[:, lanes] + update
            out_refs[0][:, lanes] = final.astype(jnp.bfloat16)


def run_stage(flags, timesteps, x, noise, vectors, prompts, weights, last, cols, head_width, tokens, tiles, mode, level, group, partial):
    noised = noise is not None
    width = weights.shape[2]
    positions = x[0].shape[0] if mode == 2 else x[0].shape[1] * tiles
    rows = weights.shape[1]
    vmem = pl.BlockSpec(memory_space=pltpu.VMEM)
    smem = pl.BlockSpec(memory_space=pltpu.SMEM)
    inputs = list(x) + (noise if noised else []) + list(vectors) + [prompts, weights, last]
    spare = (positions, width)
    return pl.pallas_call(
        functools.partial(
            stage_kernel, cols, head_width, tokens, tiles, len(x), mode, level if noised else 0,
            group, partial,
        ),
        in_specs=[smem, smem] + [vmem] * len(inputs),
        out_specs=[vmem],
        out_shape=[jax.ShapeDtypeStruct((positions, width), jnp.bfloat16)],
        scratch_shapes=[
            pltpu.VMEM((3, rows, positions), jnp.bfloat16),
            pltpu.VMEM((positions, width), jnp.float32),
            pltpu.VMEM((positions, width), jnp.bfloat16),
            pltpu.VMEM((positions, rows), jnp.bfloat16),
            pltpu.VMEM(spare if mode != 2 else (16, LANES), jnp.bfloat16),
            pltpu.VMEM(spare if noised else (16, LANES), jnp.bfloat16),
        ],
        compiler_params=pltpu.CompilerParams(vmem_limit_bytes=24 * 2**20),
    )(flags, timesteps, *inputs)[0]


def per_device(
    latents,
    prompt_tokens,
    fresh_noise,
    timesteps,
    entry_order,
    timestep_weight,
    conv_kernel,
    norm_gain,
    layer_norm_bias,
    qkv_weight,
    prompt_weight,
    out_weight,
):
    sections = lax.axis_size("section")
    tiles = lax.axis_size("tile")
    parts = lax.axis_size("batch")
    section = lax.axis_index("section")
    tile = lax.axis_index("tile")
    micro, rows_here, cols, width = latents.shape
    steps = timesteps.shape[0]
    head_width = width // HEADS
    span = qkv_weight.shape[3]
    tokens = prompt_tokens.shape[1]
    assert micro == tiles and tiles & (tiles - 1) == 0

    features = time_features(timesteps, timestep_weight.shape[1] // 2)
    temb = jnp.dot(features, timestep_weight[0], preferred_element_type=jnp.float32)

    own_qkv = qkv_weight[0].transpose(1, 2, 0)
    own_out = out_weight[0]
    paired = parts % 2 == 0
    parity = lax.axis_index("batch") % 2 if paired else jnp.int32(0)
    flags = jnp.stack([section, tile, parity]).astype(jnp.int32)

    def exchanged(source, axis, mask):
        moved = []
        for piece in source:
            moved.append(swapped(piece, axis, mask))
        return moved

    halves = list(cut(flags, 0, own_qkv, own_out))
    halves, own_qkv, own_out, prompt_tokens, latents, fresh_noise = lax.optimization_barrier(
        (halves, own_qkv, own_out, prompt_tokens, latents, fresh_noise)
    )

    def picked(stack):
        return [lax.dynamic_index_in_dim(stack, tile ^ k, 0, False) for k in range(tiles)]

    def sent(mine, group=None):
        first = 0 if group is None else group * tiles
        pairs = [[(first + t, first + (t ^ k)) for t in range(tiles)] for k in range(tiles)]
        axis = "tile" if group is None else ("section", "tile")
        result = list(mine[:1])
        for k in range(1, tiles):
            result.append(lax.ppermute(mine[k], axis, pairs[k]))
        return result

    def across(stack, group=None):
        return sent(picked(stack), group)

    def in_order(entries):
        stacked = jnp.stack(entries)
        return jnp.stack(
            [lax.dynamic_index_in_dim(stacked, tile ^ r, 0, False) for r in range(tiles)]
        )

    padded = -(-tokens // LANES) * LANES
    prompt_rows = prompt_weight[0].transpose(1, 2, 0).reshape(2 * span, -1)

    def relayed(near, bit):
        if not paired:
            return exchanged(list(cut(flags, 1, own_qkv, own_out)), "tile", bit)
        far = []
        for piece in range(4):
            far.append(swapped(near[piece], "batch", 1))
        return far

    paired_start = tiles == 4 and sections > 1
    far_mask = tiles // 2
    slots = [None] * tiles
    near = {bit: exchanged(halves, "tile", bit) for bit in [1 << i for i in range(1, tiles.bit_length() - 1)]}
    token_rows = jnp.pad(prompt_tokens, ((0, 0), (0, padded - tokens), (0, 0)))
    prompt_local = project_prompts(token_rows, prompt_rows).reshape(micro, 2, span, padded)

    def two(stack, k):
        return jnp.stack(
            [lax.dynamic_index_in_dim(stack, tile ^ k ^ j, 0, False) for j in (0, far_mask)]
        )

    latent_rows = latents.reshape(micro * rows_here * cols, width)
    picks = picked(prompt_local)
    if paired_start:
        picks[:2] = [two(prompt_local, 0), two(prompt_local, 1)]
    moved = sent(picks, None)
    if paired_start:
        pair_prompts = [[piece[j] for piece in moved[:2]] for j in range(2)]
        prompts = [[piece[0]] for piece in moved[:2]] + [[piece] for piece in moved[2:]]
        masks = tuple((k, k ^ far_mask) for k in range(tiles))
        x = sent(pick(flags, None, latent_rows, rows_here * cols, masks, 60), 0)
    else:
        prompts = [[piece] for piece in moved]
        masks = tuple((k,) for k in range(tiles))
        x = sent(pick(flags, None, latent_rows, rows_here * cols, masks, 60), 0)
    slots[0] = [own_qkv, own_out[None]]
    if tiles > 1:
        slots[1] = exchanged(slots[0], "tile", 1)
    for bit in near:
        slots[bit] = near[bit] + relayed(near[bit], bit)
    for slot in range(3, tiles):
        bit = 1 << (slot.bit_length() - 1)
        if slot != bit:
            slots[slot] = [
                None if index % 4 == 3 else swapped(piece, "tile", slot - bit)
                for index, piece in enumerate(slots[bit])
            ]

    noises = [None]
    for level in range(1, steps):
        rows = fresh_noise[level - 1].reshape(micro * rows_here * cols, width)
        noises.append(
            pick(flags, entry_order, rows, rows_here * cols, tuple((k,) for k in range(tiles)), 16)
        )
    tembs = [temb[level : level + 1] for level in range(steps)]
    taps = conv_kernel[0]
    if paired_start:
        chip_weights, chip_last, *chip_prompts = assemble(
            flags,
            0,
            [[slots[0][:1], slots[1][:1]], [slots[0][1:], slots[1][1:]]]
            + [[[p] for p in pair] for pair in pair_prompts],
        )
        begun = []
        for j in (1, 0):
            begun.append(
                run_stage(
                    flags, timesteps, x, None,
                    [tembs[0], taps, norm_gain, layer_norm_bias],
                    chip_prompts[j], chip_weights, chip_last, cols, head_width, tokens, tiles,
                    j, 0, 0, j == 1,
                )
            )
        partner, mine = begun
        pairs = [(t, tiles + t) for t in range(tiles)]
        crossed = [(t, tiles + (t ^ far_mask)) for t in range(tiles)]
        x = [lax.ppermute(mine, ("section", "tile"), pairs)]
        x.append(lax.ppermute(partner, ("section", "tile"), crossed))

    firsts = [slot[:1] if len(slot) == 2 else slot[:3] + slot[4:7] for slot in slots]
    firsts, prompts, tembs, taps = lax.optimization_barrier((firsts, prompts, tembs, taps))
    weights = assemble(flags, None, [firsts])[0]
    for bit in near:
        slots[bit][7], weights = lax.optimization_barrier((slots[bit][7], weights))
    lasts = [None] * tiles
    for slot in range(tiles):
        bit = 1 << (slot.bit_length() - 1) if slot else 0
        if slot < 2:
            lasts[slot] = slots[slot][1:]
        elif slot == bit:
            lasts[slot] = [slots[slot][3], slots[slot][7]]
        else:
            lasts[slot] = exchanged([slots[bit][3], slots[bit][7]], "tile", slot - bit)
    last, prompts = assemble(flags, None, [lasts, prompts])
    noises = [None] + [sent(mine, 0) for mine in noises[1:]]

    stages = steps * sections
    for stage in range(1 if paired_start else 0, stages):
        level, group = divmod(stage, sections)
        noise = noises[level] if group == 0 else None
        x = run_stage(
            flags, timesteps, x, noise,
            [tembs[level], taps, norm_gain, layer_norm_bias],
            prompts, weights, last, cols, head_width, tokens, tiles, 0 if stage == 0 else 2,
            level, group, False,
        )
        if stage + 1 < stages:
            x = [lax.ppermute(x, "section", [(group, (group + 1) % sections)])]

    share = width // sections
    final = sections - 1
    mine = x[:, final * share :]
    for other in range(final):
        piece = x[:, other * share : (other + 1) * share]
        mine = jnp.where(section == other, lax.ppermute(piece, "section", [(final, other)]), mine)
    blocks = mine.reshape(tiles, rows_here, cols, share)
    return in_order(across(blocks))


def solution(mesh):
    placed = (
        P("batch", "tile", None, None),
        P("batch", None, None),
        P(None, "batch", "tile", None, None),
        P(),
        P("batch"),
        P("section", None, None),
        P("section", None, None),
        P("section", None),
        P("section", None),
        P("section", None, None, "tile"),
        P("section", None, None, "tile"),
        P("section", "tile", None),
    )

    return jax.shard_map(
        per_device,
        mesh=mesh,
        in_specs=placed,
        out_specs=P("batch", "tile", None, "section"),
        check_vma=False,
    )
```

```python
import functools
import math

import jax
import jax.numpy as jnp
from jax import lax
from jax.experimental import pallas as pl
from jax.experimental.pallas import tpu as pltpu
from jax.sharding import PartitionSpec as P


HEADS = 20
LANES = 128


def alpha_bar_at(position):
    shape = (8, LANES)
    positions = lax.broadcasted_iota(jnp.int32, shape, 0) * LANES
    positions = positions + lax.broadcasted_iota(jnp.int32, shape, 1)
    low_root = math.sqrt(0.00085)
    high_root = math.sqrt(0.012)
    roots = low_root + (high_root - low_root) * positions.astype(jnp.float32) / 999.0
    logs = jnp.where(positions <= position, jnp.log(1.0 - roots * roots), 0.0)
    return jnp.exp(jnp.sum(jnp.sum(logs, axis=1, keepdims=True), axis=0, keepdims=True))


def time_features(timesteps, half_count):
    exponents = jnp.arange(half_count, dtype=jnp.float32) / half_count
    freq_row = jnp.exp(-math.log(10000.0) * exponents)
    angles = timesteps.astype(jnp.float32)[:, None] * freq_row[None, :]
    return jnp.concatenate([jnp.cos(angles), jnp.sin(angles)], axis=1).astype(jnp.bfloat16)


def swapped(value, axis, mask):
    count = lax.axis_size(axis)
    return lax.ppermute(value, axis, [(i, i ^ mask) for i in range(count)])


def prompt_kernel(token_ref, weight_ref, out_ref):
    slots = token_ref.shape[1]
    rows = lax.dot_general(
        weight_ref[...],
        token_ref[...].reshape(2 * slots, token_ref.shape[2]),
        (((1,), (1,)), ((), ())),
        preferred_element_type=jnp.float32,
    ).astype(jnp.bfloat16)
    out_ref[0] = rows[:, :slots]
    out_ref[1] = rows[:, slots:]


def project_prompts(tokens, weight):
    count, slots, width = tokens.shape
    rows = weight.shape[0]
    return pl.pallas_call(
        prompt_kernel,
        grid=(count // 2,),
        in_specs=[
            pl.BlockSpec((2, slots, width), lambda i: (i, 0, 0)),
            pl.BlockSpec((rows, width), lambda i: (0, 0)),
        ],
        out_specs=pl.BlockSpec((2, rows, slots), lambda i: (i, 0, 0)),
        out_shape=jax.ShapeDtypeStruct((count, rows, slots), jnp.bfloat16),
        compiler_params=pltpu.CompilerParams(vmem_limit_bytes=60 * 2**20),
        name="prompts",
    )(tokens, weight)


def pick_kernel(masks, block, flag_ref, order_ref, source_ref, *refs):
    outs, sems = refs[:-1], refs[-1]
    tile = flag_ref[1]
    copies = []
    for index, out in enumerate(outs):
        for j, mask in enumerate(masks[index]):
            entry = tile ^ mask
            if order_ref is not None:
                wanted = entry
                entry = jnp.int32(0)
                for m in range(order_ref.shape[0]):
                    entry = entry + jnp.where(order_ref[m] == wanted, m, 0)
            rows = pl.ds(pl.multiple_of(entry * block, 16), block)
            copies.append(
                pltpu.make_async_copy(source_ref.at[rows], out.at[j], sems.at[index, j])
            )
    for copy in copies:
        copy.start()
    for copy in copies:
        copy.wait()


def pick(flags, order, source, block, masks, vmem_total):
    kernel = functools.partial(pick_kernel, masks, block)
    if order is None:
        kernel = lambda flag_ref, *refs: pick_kernel(masks, block, flag_ref, None, *refs)
    smem = pl.BlockSpec(memory_space=pltpu.SMEM)
    width = source.shape[1]
    return pl.pallas_call(
        kernel,
        in_specs=[smem] + ([smem] if order is not None else []) + [pl.BlockSpec(memory_space=pltpu.HBM)],
        out_specs=[pl.BlockSpec(memory_space=pltpu.VMEM)] * len(masks),
        out_shape=[jax.ShapeDtypeStruct((len(m), block, width), source.dtype) for m in masks],
        scratch_shapes=[pltpu.SemaphoreType.DMA((len(masks), len(masks[0])))],
        compiler_params=pltpu.CompilerParams(vmem_limit_bytes=vmem_total * 2**20),
    )(flags, *([order] if order is not None else []), source)


def cut_kernel(which, pieces, flag_ref, qkv_ref, last_ref, *refs):
    outs, sems = refs[:-1], refs[-1]
    half = outs[0].shape[0]
    parity = flag_ref[2] if which == 0 else 1 - flag_ref[2]
    rows = pl.ds(pl.multiple_of(parity * half, 16), half)
    copies = []
    for index, (piece, out) in enumerate(zip(pieces, outs)):
        source = qkv_ref.at[piece, rows] if piece < 3 else last_ref.at[rows]
        copies.append(pltpu.make_async_copy(source, out, sems.at[index]))
    for copy in copies:
        copy.start()
    for copy in copies:
        copy.wait()


def cut(flags, which, pieces, qkv, last):
    span, width = last.shape
    hbm = pl.BlockSpec(memory_space=pltpu.HBM)
    return pl.pallas_call(
        functools.partial(cut_kernel, which, pieces),
        in_specs=[pl.BlockSpec(memory_space=pltpu.SMEM), hbm, hbm],
        out_specs=[pl.BlockSpec(memory_space=pltpu.VMEM)] * len(pieces),
        out_shape=[jax.ShapeDtypeStruct((span // 2, width), jnp.bfloat16)] * len(pieces),
        scratch_shapes=[pltpu.SemaphoreType.DMA((len(pieces),))],
        compiler_params=pltpu.CompilerParams(vmem_limit_bytes=60 * 2**20),
        name="cut",
    )(flags, qkv, last)


def assemble_kernel(layouts, group, flag_ref, *refs):
    total = sum(sum(counts) for counts, _ in layouts)
    sources, outs, sems = refs[:total], refs[total:-1], refs[-1]
    parity = flag_ref[2]
    copies = []
    at = 0
    for out, (counts, piece_total) in zip(outs, layouts):
        span = out.shape[1] // len(counts)
        for slot, count in enumerate(counts):
            for part in range(count):
                source, sem = sources[at], sems.at[at]
                at += 1
                if count == 1:
                    target = out.at[:, pl.ds(slot * span, span)]
                else:
                    half = span // 2
                    place = parity if part < piece_total else 1 - parity
                    rows = pl.ds(pl.multiple_of(slot * span + place * half, 16), half)
                    target = out.at[part % piece_total, rows]
                copies.append(pltpu.make_async_copy(source, target, sem))

    @pl.when(flag_ref[0] == group if group is not None else flag_ref[0] >= 0)
    def _():
        for copy in copies:
            copy.start()
        for copy in copies:
            copy.wait()


def assemble(flags, group, arrays):
    layouts, sources, shapes = [], [], []
    for slots in arrays:
        piece_total, span, width = slots[0][0].shape
        layouts.append((tuple(len(slot) for slot in slots), piece_total))
        sources += [piece for slot in slots for piece in slot]
        shapes.append(jax.ShapeDtypeStruct((piece_total, span * len(slots), width), jnp.bfloat16))
    hbm = pl.BlockSpec(memory_space=pltpu.HBM)
    return pl.pallas_call(
        functools.partial(assemble_kernel, tuple(layouts), group),
        in_specs=[pl.BlockSpec(memory_space=pltpu.SMEM)] + [hbm] * len(sources),
        out_specs=[pl.BlockSpec(memory_space=pltpu.VMEM)] * len(shapes),
        out_shape=shapes,
        scratch_shapes=[pltpu.SemaphoreType.DMA((len(sources),))],
        compiler_params=pltpu.CompilerParams(vmem_limit_bytes=16 * 2**20),
    )(flags, *sources)


def stage_kernel(cols, head_width, token_total, tiles, count, mode, level, group, partial, *refs):
    noised = level > 0
    flag_ref, steps_ref = refs[:2]
    refs = refs[2:]
    x_refs, refs = refs[:count], refs[count:]
    noise_refs, refs = (refs[:tiles], refs[tiles:]) if noised else (None, refs)
    temb_ref, conv_ref, gain_ref, bias_ref, prompt_ref, weight_ref, last_ref = refs[:7]
    out_refs, refs = refs[7:-6], refs[-6:]
    proj, mixed_ref, normed_ref, heads_ref, x_ref, noise_ref = refs
    positions, width = mixed_ref.shape
    rows_total = weight_ref.shape[1]
    block = positions // tiles
    chunk_total = width // LANES

    @pl.when(flag_ref[0] == group)
    def _():
        tile = flag_ref[1]
        for k in range(tiles):
            rows = pl.ds(pl.multiple_of((tile ^ k) * block, 16), block)
            if mode in (0, 1):
                x_ref[rows] = x_refs[k][mode]
            if noised:
                noise_ref[rows] = noise_refs[k][0]
        sources = [x_ref] if mode in (0, 1) else x_refs

        if noised:
            alpha_bar = alpha_bar_at(steps_ref[level])
            keep, renew = jnp.sqrt(alpha_bar), jnp.sqrt(1.0 - alpha_bar)
        place = lax.broadcasted_iota(jnp.int32, (positions, LANES), 0) % cols
        first = place == 0
        last = place == cols - 1
        gap = jnp.zeros((cols, LANES), jnp.float32)

        def mix_chunk(index, total):
            lanes = pl.ds(pl.multiple_of(index * LANES, LANES), LANES)
            value = sources[0][:, lanes].astype(jnp.float32)
            for other in sources[1:]:
                value = (value + other[:, lanes].astype(jnp.float32)).astype(jnp.bfloat16)
                value = value.astype(jnp.float32)
            if noised:
                value = keep * value + renew * noise_ref[:, lanes].astype(jnp.float32)
                value = value.astype(jnp.bfloat16).astype(jnp.float32)
            value = (value + temb_ref[:, lanes]).astype(jnp.bfloat16).astype(jnp.float32)
            before = jnp.where(first, 0.0, pltpu.roll(value, 1, 0))
            after = jnp.where(last, 0.0, pltpu.roll(value, positions - 1, 0))
            taps = conv_ref[:, lanes]

            def row_of(a):
                return (
                    taps[3 * a : 3 * a + 1] * before
                    + taps[3 * a + 1 : 3 * a + 2] * value
                    + taps[3 * a + 2 : 3 * a + 3] * after
                )

            mixed = value + row_of(1)
            mixed = mixed + jnp.concatenate([gap, row_of(0)[: positions - cols]], axis=0)
            mixed = mixed + jnp.concatenate([row_of(2)[cols:], gap], axis=0)
            mixed_ref[:, lanes] = mixed
            return total + mixed

        total = lax.fori_loop(
            0, chunk_total, mix_chunk, jnp.zeros((positions, LANES), jnp.float32)
        )
        centre = jnp.sum(total, axis=1, keepdims=True) / width

        def spread_chunk(index, total):
            lanes = pl.ds(pl.multiple_of(index * LANES, LANES), LANES)
            return total + jnp.square(mixed_ref[:, lanes] - centre)

        total = lax.fori_loop(
            0, chunk_total, spread_chunk, jnp.zeros((positions, LANES), jnp.float32), unroll=2
        )
        scale = lax.rsqrt(jnp.sum(total, axis=1, keepdims=True) / width + 1e-05)

        def norm_chunk(index, carry):
            lanes = pl.ds(pl.multiple_of(index * LANES, LANES), LANES)
            value = (mixed_ref[:, lanes] - centre) * scale
            normed_ref[:, lanes] = (value * gain_ref[:, lanes] + bias_ref[:, lanes]).astype(
                jnp.bfloat16
            )
            return carry

        lax.fori_loop(0, chunk_total, norm_chunk, 0, unroll=2)

        big = rows_total // 2
        for piece in range(3):
            for start in range(0, rows_total, big):
                rows = pl.ds(start, big)
                proj[piece, rows] = lax.dot_general(
                    weight_ref[piece, rows],
                    normed_ref[...],
                    (((1,), (1,)), ((), ())),
                    preferred_element_type=jnp.float32,
                ).astype(jnp.bfloat16)

        prompt_slots = prompt_ref.shape[2]
        pair = 2 * head_width
        usable = lax.broadcasted_iota(jnp.int32, (2 * positions, prompt_slots), 1) < token_total
        upper = lax.broadcasted_iota(jnp.int32, (positions, pair), 1) < head_width
        factor = 1.0 / math.sqrt(head_width)

        def pair_step(index, carry):
            rows = pl.ds(pl.multiple_of(index * pair, pair), pair)
            both = proj[0, rows].T
            nothing = jnp.zeros_like(both)
            queries = jnp.concatenate(
                [jnp.where(upper, both, nothing), jnp.where(upper, nothing, both)], axis=0
            )
            keys = jnp.concatenate([proj[1, rows], prompt_ref[0, rows]], axis=1)
            values = jnp.concatenate([proj[2, rows], prompt_ref[1, rows]], axis=1)
            scores = jnp.dot(queries, keys, preferred_element_type=jnp.float32)
            powers = jnp.exp(scores * factor)
            front = powers[:, :positions]
            rear = jnp.where(usable, powers[:, positions:], 0.0)
            if front.shape == rear.shape:
                whole = jnp.sum(front + rear, axis=1, keepdims=True)
            else:
                whole = jnp.sum(front, axis=1, keepdims=True) + jnp.sum(rear, axis=1, keepdims=True)
            inverse = 1.0 / whole
            soft = jnp.concatenate([front * inverse, rear * inverse], axis=1).astype(jnp.bfloat16)
            joined = lax.dot_general(
                soft, values, (((1,), (1,)), ((), ())), preferred_element_type=jnp.float32
            )
            heads_ref[:, rows] = jnp.where(upper, joined[:positions], joined[positions:]).astype(
                jnp.bfloat16
            )
            return carry

        lax.fori_loop(0, rows_total // pair, pair_step, 0, unroll=min(10, rows_total // pair))

        piece = 2 * LANES
        for start in range(0, width, piece):
            lanes = pl.ds(start, piece)
            update = jnp.dot(
                heads_ref[...], last_ref[0, :, lanes], preferred_element_type=jnp.float32
            )
            final = update if partial else mixed_ref[:, lanes] + update
            out_refs[0][:, lanes] = final.astype(jnp.bfloat16)


def run_stage(flags, timesteps, x, noise, vectors, prompts, weights, last, cols, head_width, tokens, tiles, mode, level, group, partial):
    noised = noise is not None
    width = weights.shape[2]
    positions = x[0].shape[0] if mode == 2 else x[0].shape[1] * tiles
    rows = weights.shape[1]
    vmem = pl.BlockSpec(memory_space=pltpu.VMEM)
    smem = pl.BlockSpec(memory_space=pltpu.SMEM)
    inputs = list(x) + (noise if noised else []) + list(vectors) + [prompts, weights, last]
    spare = (positions, width)
    return pl.pallas_call(
        functools.partial(
            stage_kernel, cols, head_width, tokens, tiles, len(x), mode, level if noised else 0,
            group, partial,
        ),
        in_specs=[smem, smem] + [vmem] * len(inputs),
        out_specs=[vmem],
        out_shape=[jax.ShapeDtypeStruct((positions, width), jnp.bfloat16)],
        scratch_shapes=[
            pltpu.VMEM((3, rows, positions), jnp.bfloat16),
            pltpu.VMEM((positions, width), jnp.float32),
            pltpu.VMEM((positions, width), jnp.bfloat16),
            pltpu.VMEM((positions, rows), jnp.bfloat16),
            pltpu.VMEM(spare if mode != 2 else (16, LANES), jnp.bfloat16),
            pltpu.VMEM(spare if noised else (16, LANES), jnp.bfloat16),
        ],
        compiler_params=pltpu.CompilerParams(vmem_limit_bytes=24 * 2**20),
    )(flags, timesteps, *inputs)[0]


def per_device(
    latents,
    prompt_tokens,
    fresh_noise,
    timesteps,
    entry_order,
    timestep_weight,
    conv_kernel,
    norm_gain,
    layer_norm_bias,
    qkv_weight,
    prompt_weight,
    out_weight,
):
    sections = lax.axis_size("section")
    tiles = lax.axis_size("tile")
    parts = lax.axis_size("batch")
    section = lax.axis_index("section")
    tile = lax.axis_index("tile")
    micro, rows_here, cols, width = latents.shape
    steps = timesteps.shape[0]
    head_width = width // HEADS
    span = qkv_weight.shape[3]
    tokens = prompt_tokens.shape[1]
    assert micro == tiles and tiles & (tiles - 1) == 0

    features = time_features(timesteps, timestep_weight.shape[1] // 2)
    temb = jnp.dot(features, timestep_weight[0], preferred_element_type=jnp.float32)

    own_qkv = qkv_weight[0].transpose(1, 2, 0)
    own_out = out_weight[0]
    paired = parts % 2 == 0
    parity = lax.axis_index("batch") % 2 if paired else jnp.int32(0)
    flags = jnp.stack([section, tile, parity]).astype(jnp.int32)

    def exchanged(source, axis, mask):
        moved = []
        for piece in source:
            moved.append(swapped(piece, axis, mask))
        return moved

    halves = list(cut(flags, 0, (0, 1, 2, 3), own_qkv, own_out))
    halves, own_qkv, own_out, prompt_tokens, latents, fresh_noise = lax.optimization_barrier(
        (halves, own_qkv, own_out, prompt_tokens, latents, fresh_noise)
    )

    def picked(stack):
        return [lax.dynamic_index_in_dim(stack, tile ^ k, 0, False) for k in range(tiles)]

    def sent(mine, group=None):
        first = 0 if group is None else group * tiles
        pairs = [[(first + t, first + (t ^ k)) for t in range(tiles)] for k in range(tiles)]
        axis = "tile" if group is None else ("section", "tile")
        result = list(mine[:1])
        for k in range(1, tiles):
            result.append(lax.ppermute(mine[k], axis, pairs[k]))
        return result

    def across(stack, group=None):
        return sent(picked(stack), group)

    def in_order(entries):
        stacked = jnp.stack(entries)
        return jnp.stack(
            [lax.dynamic_index_in_dim(stacked, tile ^ r, 0, False) for r in range(tiles)]
        )

    padded = -(-tokens // LANES) * LANES
    prompt_rows = prompt_weight[0].transpose(1, 2, 0).reshape(2 * span, -1)

    def relayed(near, bit):
        if not paired:
            return exchanged(list(cut(flags, 1, (0, 1, 2, 3), own_qkv, own_out)), "tile", bit)
        far = []
        for piece in range(4):
            far.append(swapped(near[piece], "batch", 1))
        return far

    paired_start = tiles == 4 and sections > 1
    far_mask = tiles // 2
    slots = [None] * tiles
    near = {bit: exchanged(halves, "tile", bit) for bit in [1 << i for i in range(1, tiles.bit_length() - 1)]}
    token_rows = jnp.pad(prompt_tokens, ((0, 0), (0, padded - tokens), (0, 0)))
    prompt_local = project_prompts(token_rows, prompt_rows).reshape(micro, 2, span, padded)

    def two(stack, k):
        return jnp.stack(
            [lax.dynamic_index_in_dim(stack, tile ^ k ^ j, 0, False) for j in (0, far_mask)]
        )

    latent_rows = latents.reshape(micro * rows_here * cols, width)
    picks = picked(prompt_local)
    if paired_start:
        picks[:2] = [two(prompt_local, 0), two(prompt_local, 1)]
    moved = sent(picks, None)
    if paired_start:
        pair_prompts = [[piece[j] for piece in moved[:2]] for j in range(2)]
        prompts = [[piece[0]] for piece in moved[:2]] + [[piece] for piece in moved[2:]]
        masks = tuple((k, k ^ far_mask) for k in range(tiles))
        x = sent(pick(flags, None, latent_rows, rows_here * cols, masks, 60), 0)
    else:
        prompts = [[piece] for piece in moved]
        masks = tuple((k,) for k in range(tiles))
        x = sent(pick(flags, None, latent_rows, rows_here * cols, masks, 60), 0)
    slots[0] = [own_qkv, own_out[None]]
    if tiles > 1:
        slots[1] = exchanged(slots[0], "tile", 1)
    for bit in near:
        slots[bit] = near[bit] + relayed(near[bit], bit)
    for slot in range(3, tiles):
        bit = 1 << (slot.bit_length() - 1)
        if slot != bit:
            slots[slot] = []
            for index, piece in enumerate(slots[bit]):
                slots[slot].append(None if index % 4 == 3 else swapped(piece, "tile", slot - bit))

    noises = [None]
    for level in range(1, steps):
        rows = fresh_noise[level - 1].reshape(micro * rows_here * cols, width)
        noises.append(
            pick(flags, entry_order, rows, rows_here * cols, tuple((k,) for k in range(tiles)), 16)
        )
    tembs = [temb[level : level + 1] for level in range(steps)]
    taps = conv_kernel[0]
    if paired_start:
        chip_weights, chip_last, *chip_prompts = assemble(
            flags,
            0,
            [[slots[0][:1], slots[1][:1]], [slots[0][1:], slots[1][1:]]]
            + [[[p] for p in pair] for pair in pair_prompts],
        )
        begun = []
        for j in (1, 0):
            begun.append(
                run_stage(
                    flags, timesteps, x, None,
                    [tembs[0], taps, norm_gain, layer_norm_bias],
                    chip_prompts[j], chip_weights, chip_last, cols, head_width, tokens, tiles,
                    j, 0, 0, j == 1,
                )
            )
        partner, mine = begun
        pairs = [(t, tiles + t) for t in range(tiles)]
        crossed = [(t, tiles + (t ^ far_mask)) for t in range(tiles)]
        x = [lax.ppermute(mine, ("section", "tile"), pairs)]
        x.append(lax.ppermute(partner, ("section", "tile"), crossed))

    firsts = [slot[:1] if len(slot) == 2 else slot[:3] + slot[4:7] for slot in slots]
    firsts, prompts, tembs, taps = lax.optimization_barrier((firsts, prompts, tembs, taps))
    weights = assemble(flags, None, [firsts])[0]
    for bit in near:
        slots[bit][7], weights = lax.optimization_barrier((slots[bit][7], weights))
    lasts = [None] * tiles
    for slot in range(tiles):
        bit = 1 << (slot.bit_length() - 1) if slot else 0
        if slot < 2:
            lasts[slot] = slots[slot][1:]
        elif slot == bit:
            lasts[slot] = [slots[slot][3], slots[slot][7]]
        else:
            lasts[slot] = exchanged([slots[bit][3], slots[bit][7]], "tile", slot - bit)
    last, prompts = assemble(flags, None, [lasts, prompts])
    noises = [None] + [sent(mine, 0) for mine in noises[1:]]

    stages = steps * sections
    for stage in range(1 if paired_start else 0, stages):
        level, group = divmod(stage, sections)
        noise = noises[level] if group == 0 else None
        x = run_stage(
            flags, timesteps, x, noise,
            [tembs[level], taps, norm_gain, layer_norm_bias],
            prompts, weights, last, cols, head_width, tokens, tiles, 0 if stage == 0 else 2,
            level, group, False,
        )
        if stage + 1 < stages:
            x = [lax.ppermute(x, "section", [(group, (group + 1) % sections)])]

    share = width // sections
    final = sections - 1
    mine = x[:, final * share :]
    for other in range(final):
        piece = x[:, other * share : (other + 1) * share]
        mine = jnp.where(section == other, lax.ppermute(piece, "section", [(final, other)]), mine)
    blocks = mine.reshape(tiles, rows_here, cols, share)
    return in_order(across(blocks))


def solution(mesh):
    placed = (
        P("batch", "tile", None, None),
        P("batch", None, None),
        P(None, "batch", "tile", None, None),
        P(),
        P("batch"),
        P("section", None, None),
        P("section", None, None),
        P("section", None),
        P("section", None),
        P("section", None, None, "tile"),
        P("section", None, None, "tile"),
        P("section", "tile", None),
    )

    return jax.shard_map(
        per_device,
        mesh=mesh,
        in_specs=placed,
        out_specs=P("batch", "tile", None, "section"),
        check_vma=False,
    )
```
